32 devices in a mesh: ctx: 16 (over z, y, x), head: 2 (over core).
Axes of the slice: x: 2, y: 2, z: 4, core: 2. Of those that a mesh axis runs over, the one named last changes fastest.
Arguments:
- hidden: bfloat16 [256, 8192], P(None, 'ctx'), may hold values from -6 to 6
- q_weight: bfloat16 [8192, 8192], P('ctx', 'head'), may hold values from -0.0625 to 0.0625
- keys: bfloat16 [8, 32768, 128], P('head', 'ctx'), may hold values from -400 to 400
- values: bfloat16 [8, 32768, 128], P('head', 'ctx'), may hold values from -6 to 6
- o_weight: bfloat16 [8192, 8192], P('head', 'ctx'), may hold values from -0.0625 to 0.0625
- start: int32 [1], replicated, may hold values from 0 to 32512
Outputs:
- importance: float32 [8, 32768], P('head', 'ctx')
- mixed: bfloat16 [256, 8192], P('head', 'ctx')
The draws below stay inside these ranges and needn't reach their ends.
All inputs are finite; a program needn't handle non-finite values.
Results may differ from the reference program's by a relative error of at most 0.035.
Values may be sent and summed in bfloat16 or wider, within the bound.
No kernel may reach another device: no remote copies, remote signals or barrier semaphores. Data moves between devices by JAX's collectives and lax.ppermute only.
A program may use at most 64 MiB of HBM per device.

```python
import jax
import jax.numpy as jnp
from jax import lax

D = 8192
QUERY_HEADS = 64
KEY_VALUE_HEADS = 8
HEAD_DIMENSION = 128
REPEAT_ROWS = 256
CACHED_SLOTS = 32768


def draw_keys(key, part):
    key_first_part = jax.random.fold_in(jax.random.fold_in(key, 7), 0)
    base_offset = jax.random.normal(key_first_part, (KEY_VALUE_HEADS, CACHED_SLOTS, HEAD_DIMENSION), jnp.float32)
    return jnp.clip(base_offset, -400.0, 400.0).astype(jnp.bfloat16)


def steps_of(stream_key, shape, pieces, least, high):
    gain, own = 1.0, jax.random.fold_in(stream_key, 6)
    for axis_at, blocks in pieces:
        heights = jnp.exp(jax.random.uniform(jax.random.fold_in(own, axis_at), (blocks,), jnp.float32, least / len(pieces), high / len(pieces)))
        gain = gain * jnp.repeat(heights, shape[axis_at] // blocks).reshape([-1 if axis == axis_at else 1 for axis in range(len(shape))])
    return gain


def noise(key, dims, scale, bound, cuts=(), held_as=jnp.bfloat16):
    result = scale * jax.random.normal(key, dims, jnp.float32)
    if cuts:
        result = result * steps_of(key, dims, cuts, -0.22, 0.18)
    return jnp.clip(result, -bound, bound).astype(held_as)


def setup_inputs(seed: int = 0) -> dict:
    splits = jax.random.split(jax.random.key(seed), 7)
    hidden = noise(splits[0], (REPEAT_ROWS, D), 1.0, 6.0, ((1, 16),))
    q_weight = noise(splits[1], (D, QUERY_HEADS * HEAD_DIMENSION), D ** -0.5, 0.0625, ((0, 16), (1, 2)))
    keys = draw_keys(jax.random.fold_in(splits[6], 71), 0)
    values = noise(splits[3], (KEY_VALUE_HEADS, CACHED_SLOTS, HEAD_DIMENSION), 1.0, 6.0, ((0, 2), (1, 16)))
    o_weight = noise(splits[4], (QUERY_HEADS * HEAD_DIMENSION, D), (QUERY_HEADS * HEAD_DIMENSION) ** -0.5, 0.0625, ((0, 2), (1, 16)))
    start = jax.random.randint(splits[5], (1,), 0, CACHED_SLOTS - REPEAT_ROWS + 1).astype(jnp.int32)
    return dict(hidden=hidden, q_weight=q_weight, keys=keys, values=values, o_weight=o_weight, start=start)


NEG = -1e30


def reference(hidden, q_weight, keys, values, o_weight, start):
    head_group = QUERY_HEADS // KEY_VALUE_HEADS
    block_rows = head_group * REPEAT_ROWS
    scale = HEAD_DIMENSION ** -0.5
    query_rows = jnp.dot(hidden, q_weight, preferred_element_type=jnp.float32).astype(jnp.bfloat16)
    query_rows = query_rows.reshape(REPEAT_ROWS, KEY_VALUE_HEADS, head_group, HEAD_DIMENSION).transpose(1, 2, 0, 3).reshape(KEY_VALUE_HEADS, block_rows, HEAD_DIMENSION)
    rowpos = start[0] + jnp.tile(jnp.arange(REPEAT_ROWS, dtype=jnp.int32), head_group)
    width = min(2048, CACHED_SLOTS)
    count = CACHED_SLOTS // width
    blocks = jnp.arange(count, dtype=jnp.int32)

    def per_head(item):
        qh, kh, vh = item
        kb = kh.reshape(count, width, HEAD_DIMENSION)
        vb = vh.reshape(count, width, HEAD_DIMENSION)

        def scores(kblk, b):
            s = jnp.dot(qh, kblk.T, preferred_element_type=jnp.float32) * scale
            keypos = b * width + jnp.arange(width, dtype=jnp.int32)
            return s, keypos[None, :] <= rowpos[:, None]

        def first(carry, item2):
            kblk, b = item2
            s, mask = scores(kblk, b)
            newm = jnp.maximum(carry[0], jnp.max(jnp.where(mask, s, NEG), axis=1))
            total = carry[1] * jnp.exp(carry[0] - newm) + jnp.sum(jnp.where(mask, jnp.exp(s - newm[:, None]), 0.0), axis=1)
            return (newm, total), None

        init = (jnp.full((block_rows,), NEG, jnp.float32), jnp.zeros((block_rows,), jnp.float32))
        (peak, total), _ = lax.scan(first, init, (kb, blocks))

        def second(running_total, item2):
            kblk, vblk, b = item2
            s, mask = scores(kblk, b)
            prob = jnp.where(mask, jnp.exp(s - peak[:, None]) / total[:, None], 0.0)
            running_total = running_total + jnp.dot(prob.astype(jnp.bfloat16), vblk, preferred_element_type=jnp.float32)
            return running_total, jnp.max(prob, axis=0)

        running_total, imp = lax.scan(second, jnp.zeros((block_rows, HEAD_DIMENSION), jnp.float32), (kb, vb, blocks))
        return running_total, imp.reshape(CACHED_SLOTS)

    running_total, imp = lax.map(per_head, (query_rows, keys, values))
    attended_weight = running_total.astype(jnp.bfloat16).reshape(KEY_VALUE_HEADS, head_group, REPEAT_ROWS, HEAD_DIMENSION).transpose(2, 0, 1, 3).reshape(REPEAT_ROWS, QUERY_HEADS * HEAD_DIMENSION)
    mixed = jnp.dot(attended_weight, o_weight, preferred_element_type=jnp.float32).astype(jnp.bfloat16)
    importance = (start[0] + REPEAT_ROWS).astype(jnp.float32) * imp
    return importance, mixed
```

```python
import functools
import math

import jax
import jax.numpy as jnp
from jax import lax
from jax.experimental import pallas as pl
from jax.experimental.pallas import tpu as pltpu
from jax.sharding import PartitionSpec as P

NEG = -1e30
BF = jnp.bfloat16
F32 = jnp.float32
LANES = 128


def digits_of(n):
    out, shift = [], 0
    while n > 1:
        r = 4 if n % 4 == 0 else 2
        out.append((r, shift))
        n //= r
        shift += r.bit_length() - 1
    return out


def swap(x, axis, v):
    n = lax.axis_size(axis)
    return lax.ppermute(x, axis, [(i, i ^ v) for i in range(n)])


def block_order(digits):
    order = [0]
    for r, shift in reversed(digits):
        order = [(v << shift) | o for v in range(r) for o in order]
    return order


def gather_rows(x, axis, digits, base):
    for r, shift in reversed(digits):
        x = jnp.concatenate([x] + [swap(x, axis, v << (shift + base)) for v in range(1, r)])
    return x


def permuted_rows(x, index, order):
    blocks = x.reshape(len(order), x.shape[0] // len(order), x.shape[1])
    return jnp.concatenate(
        [lax.dynamic_index_in_dim(blocks, index ^ o, 0, False) for o in order]
    )


def cdot(a, b, ca, cb):
    return lax.dot_general(a, b, (((ca,), (cb,)), ((), ())), preferred_element_type=F32)


def project_kernel(s_ref, h_ref, w_ref, o_ref):
    o_ref[...] = jnp.dot(h_ref[...], w_ref[...], preferred_element_type=F32).astype(o_ref.dtype)


def project(block, hidden, weight, width, dtype):
    rows, k = hidden.shape
    return pl.pallas_call(
        project_kernel,
        out_shape=jax.ShapeDtypeStruct((rows, width), dtype),
        grid_spec=pltpu.PrefetchScalarGridSpec(
            num_scalar_prefetch=1,
            grid=(1,),
            in_specs=[
                pl.BlockSpec((rows, k), lambda i, s: (0, 0)),
                pl.BlockSpec((k, width), lambda i, s: (0, s[0])),
            ],
            out_specs=pl.BlockSpec((rows, width), lambda i, s: (0, 0)),
        ),
        name="query_projection",
    )(block, hidden, weight)


def visible(s, base, limit_ref):
    pos = lax.broadcasted_iota(jnp.int32, s.shape, 0) + base
    return jnp.where(pos <= limit_ref[0:1, :], s, NEG)


def attend_kernel(n_src, per, bk, span, c, s_ref, q_ref, lim_ref, *refs):
    ks, vs = refs[:n_src], refs[n_src : 2 * n_src]
    o_ref, acc, peak, stat = refs[2 * n_src :]
    d = LANES
    heads = q_ref.shape[1] // d
    ones = jnp.ones((16, bk), BF)

    for first in range(0, heads, per):
        for j in range(per):
            acc[j] = jnp.zeros(acc.shape[1:], F32)
            peak[j] = jnp.full(peak.shape[1:], NEG, F32)

        def block(src, kb, masked):
            k = ks[src][pl.ds(pl.multiple_of(kb * bk, bk), bk), :]
            vt = jnp.concatenate([vs[src][kb], ones])
            for j in range(per):
                g = first + j
                s = cdot(k, q_ref[:, g * d : (g + 1) * d], 1, 1)
                if masked:
                    s = visible(s, s_ref[2 * n_src + src] + kb * bk, lim_ref)
                old = peak[j, 0:1, :]
                new = jnp.maximum(old, jnp.max(s, axis=0, keepdims=True))
                p = jnp.exp2((s - new) * c).astype(BF)
                acc[j] = acc[j] * jnp.exp2((old - new) * c) + cdot(vt, p, 1, 0)
                peak[j, 0:1, :] = new

        for src in range(n_src):
            full, some = s_ref[src], s_ref[n_src + src]
            lax.fori_loop(0, full, lambda kb, x: (block(src, kb, False), x)[1], 0)
            lax.fori_loop(full, some, lambda kb, x: (block(src, kb, True), x)[1], 0)

        for j in range(per):
            g = first + j
            total = jnp.maximum(acc[j, d : d + 1, :], 1e-30)
            out = acc[j, 0:d, :] / total
            o_ref[:, g * d : (g + 1) * d] = out.T.astype(BF)
            stat[g : g + 1, :] = peak[j, 0:1, :] * c + jnp.log2(total)

    level = stat[...]
    hi = level.astype(BF).astype(F32)
    mid = (level - hi).astype(BF).astype(F32)
    low = level - hi - mid
    pad = jnp.zeros((d - 3 * heads, span), F32)
    o_ref[:, heads * d : (heads + 1) * d] = jnp.concatenate([hi, mid, low, pad]).T.astype(BF)


def attend(scal, q, limit, ks, vs, bk, c):
    span, width = q.shape
    heads, n_src = width // LANES, len(ks)
    per = min(4, heads)
    keys = ks[0].shape[0] * n_src
    vm = pl.BlockSpec(memory_space=pltpu.VMEM)
    return pl.pallas_call(
        functools.partial(attend_kernel, n_src, per, bk, span, c),
        out_shape=jax.ShapeDtypeStruct((span, width + LANES), BF),
        in_specs=[pl.BlockSpec(memory_space=pltpu.SMEM)] + [vm] * (2 + 2 * n_src),
        out_specs=vm,
        scratch_shapes=[
            pltpu.VMEM((per, LANES + 16, span), F32),
            pltpu.VMEM((per, 8, span), F32),
            pltpu.VMEM((heads, span), F32),
        ],
        cost_estimate=pl.CostEstimate(
            flops=4 * span * heads * LANES * keys,
            transcendentals=span * heads * keys,
            bytes_accessed=2 * span * width * 2 + 4 * keys * LANES,
        ),
        name="attend",
    )(scal, q, limit, *ks, *vs)


def merge_kernel(heads, *refs):
    srcs, o_ref = refs[:-1], refs[-1]
    d = LANES

    def level_of(r):
        parts = r[:, heads * d : (heads + 1) * d].astype(F32)
        return parts + pltpu.roll(parts, d - heads, 1) + pltpu.roll(parts, d - 2 * heads, 1)

    levels = [level_of(r) for r in srcs]
    top = functools.reduce(jnp.maximum, levels)
    weights = [jnp.exp2(x - top) for x in levels]
    total = functools.reduce(jnp.add, weights)
    weights = [w / total for w in weights]
    for g in range(heads):
        o_ref[:, g * d : (g + 1) * d] = functools.reduce(
            jnp.add,
            [w[:, g : g + 1] * r[:, g * d : (g + 1) * d].astype(F32) for w, r in zip(weights, srcs)],
        ).astype(BF)
    level = top + jnp.log2(total)
    lane = lax.broadcasted_iota(jnp.int32, level.shape, 1)
    level = jnp.where(lane < heads, level, 0.0)
    hi = level.astype(BF).astype(F32)
    mid = (level - hi).astype(BF).astype(F32)
    low = level - hi - mid
    o_ref[:, heads * d : (heads + 1) * d] = (
        hi + pltpu.roll(mid, heads, 1) + pltpu.roll(low, 2 * heads, 1)
    ).astype(BF)


def merge(parts):
    shape = parts[0].shape
    return pl.pallas_call(
        functools.partial(merge_kernel, shape[1] // LANES - 1),
        out_shape=jax.ShapeDtypeStruct(shape, BF),
        name="merge",
    )(*parts)


def importance_kernel(n_src, bk, c, s_ref, q_ref, a_ref, lim_ref, *refs):
    ks, o_ref, lev = refs[:n_src], refs[n_src], refs[n_src + 1]
    d = LANES
    heads = q_ref.shape[1] // d
    parts = a_ref[:, heads * d : (heads + 1) * d].astype(F32).T
    level = parts[0:heads] + parts[heads : 2 * heads] + parts[2 * heads : 3 * heads]
    lev[...] = level * (1.0 / c)
    factor = s_ref[3 * n_src].astype(F32)
    o_ref[...] = jnp.zeros(o_ref.shape, F32)

    def block(src, kb, masked):
        k = ks[src][pl.ds(pl.multiple_of(kb * bk, bk), bk), :]
        best = None
        for g in range(heads):
            s = cdot(k, q_ref[:, g * d : (g + 1) * d], 1, 1) - lev[g : g + 1, :]
            best = s if best is None else jnp.maximum(best, s)
        if masked:
            best = visible(best, s_ref[2 * n_src + src] + kb * bk, lim_ref)
        best = functools.reduce(
            jnp.maximum, [best[:, x : x + d] for x in range(0, best.shape[1], d)]
        )
        best = jnp.max(best.T, axis=0, keepdims=True)
        o_ref[src, pl.ds(kb, 1), :] = factor * jnp.exp2(best * c)

    for src in range(n_src):
        full, some = s_ref[src], s_ref[n_src + src]
        lax.fori_loop(0, full, lambda kb, x: (block(src, kb, False), x)[1], 0)
        lax.fori_loop(full, some, lambda kb, x: (block(src, kb, True), x)[1], 0)


def importance_of(scal, q, attended, limit, ks, bk, c):
    span, width = q.shape
    heads, n_src = width // LANES, len(ks)
    per_src = ks[0].shape[0]
    vm = pl.BlockSpec(memory_space=pltpu.VMEM)
    return pl.pallas_call(
        functools.partial(importance_kernel, n_src, bk, c),
        out_shape=jax.ShapeDtypeStruct((n_src, per_src // bk, bk), F32),
        in_specs=[pl.BlockSpec(memory_space=pltpu.SMEM)] + [vm] * (3 + n_src),
        out_specs=vm,
        scratch_shapes=[pltpu.VMEM((heads, span), F32)],
        cost_estimate=pl.CostEstimate(
            flops=2 * span * heads * LANES * per_src * n_src,
            transcendentals=per_src * n_src,
            bytes_accessed=2 * span * width * 2 + 2 * per_src * n_src * LANES,
        ),
        name="importance",
    )(scal, q, attended, limit, *ks)


def output_kernel(s_ref, a_ref, w_ref, c_ref, o_ref):
    o_ref[...] = c_ref[...] + jnp.dot(a_ref[...], w_ref[...], preferred_element_type=F32)


def output_kernel_first(s_ref, a_ref, w_ref, o_ref):
    o_ref[...] = jnp.dot(a_ref[...], w_ref[...], preferred_element_type=F32)


def output_part(block, attended, weight, width, carry):
    rows = attended.shape[0]
    cols = weight.shape[1]
    specs = [
        pl.BlockSpec((rows, width), lambda i, s: (0, 0)),
        pl.BlockSpec((width, cols), lambda i, s: (s[0], 0)),
    ]
    whole = pl.BlockSpec((rows, cols), lambda i, s: (0, 0))
    return pl.pallas_call(
        output_kernel_first if carry is None else output_kernel,
        out_shape=jax.ShapeDtypeStruct((rows, cols), F32),
        grid_spec=pltpu.PrefetchScalarGridSpec(
            num_scalar_prefetch=1,
            grid=(1,),
            in_specs=specs + ([] if carry is None else [whole]),
            out_specs=whole,
        ),
        name="output_projection",
    )(block, attended, weight, *([] if carry is None else [carry]))


def on_device(hidden, q_weight, keys, values, o_weight, start):
    span = hidden.shape[0]
    group, s_dev, head_size = keys.shape
    n = lax.axis_size("ctx")
    nh = lax.axis_size("head")
    width = q_weight.shape[1] // group
    scale = head_size**-0.5
    c = scale * math.log2(math.e)
    base = group.bit_length() - 1
    here = lax.axis_index("ctx")
    mine, outer = here % group, here // group
    digits = digits_of(n // group)
    order = block_order(digits)
    bk = min(512, s_dev)

    rows_here = permuted_rows(hidden, outer, order)
    row_index = permuted_rows(
        jnp.arange(span, dtype=jnp.int32)[:, None], outer, order
    ).reshape(1, span)
    limit = jnp.broadcast_to(start[0] + row_index, (8, span))

    def block_id(v):
        return (mine ^ v).astype(jnp.int32).reshape(1)

    parts = [
        project(block_id(v), rows_here, q_weight, width, BF if v else F32)
        for v in list(range(1, group)) + [0]
    ]
    got = [swap(parts[v - 1], "ctx", v) for v in range(1, group)]
    query = functools.reduce(jnp.add, [g.astype(F32) for g in got], parts[-1])

    count = s_dev // bk
    value_t = values.reshape(group, count, bk, head_size).transpose(0, 1, 3, 2)
    k_own = lax.dynamic_index_in_dim(keys, mine, 0, False)
    v_own = lax.dynamic_index_in_dim(value_t, mine, 0, False)
    sends = [lax.dynamic_index_in_dim(keys, mine ^ v, 0, False) for v in range(1, group)]
    vsends = [lax.dynamic_index_in_dim(value_t, mine ^ v, 0, False) for v in range(1, group)]
    query, sends, vsends = lax.optimization_barrier((query, sends, vsends))
    ks = [k_own] + [swap(x, "ctx", v + 1) for v, x in enumerate(sends)]
    vs = [v_own] + [swap(x, "ctx", v + 1) for v, x in enumerate(vsends)]

    for r, shift in digits:
        pieces = jnp.split(query, r)
        got = [swap(pieces[v].astype(BF), "ctx", v << (shift + base)) for v in range(1, r)]
        query = functools.reduce(jnp.add, [g.astype(F32) for g in got], pieces[0])
    query = gather_rows(query.astype(BF), "ctx", digits, base)

    offsets = jnp.stack([(here ^ v) * s_dev for v in range(group)]).astype(jnp.int32)
    reach = start[0] - offsets
    full = jnp.clip((reach + 1) // bk, 0, count)
    some = jnp.clip((reach + span - 1) // bk + 1, 0, count)
    scal = jnp.concatenate([full, some, offsets, start + span]).astype(jnp.int32)

    part = attend(scal, query, limit, ks, vs, bk, c)
    for r, shift in digits:
        pieces = jnp.split(part, r)
        got = [swap(pieces[v], "ctx", v << (shift + base)) for v in range(1, r)]
        part = merge([pieces[0]] + got)
    attended = gather_rows(part, "ctx", digits, base)

    own = attended[:, :width]
    arrived = [own] + [swap(own, "ctx", v) for v in range(1, group)]
    scores = importance_of(scal, query, attended, limit, ks, bk, c)
    pieces = [scores[v].reshape(1, s_dev) for v in range(group)]
    pieces = [pieces[0]] + [swap(pieces[v], "ctx", v) for v in range(1, group)]
    pieces = jnp.concatenate(pieces)
    importance = (
        jnp.concatenate(
            [lax.dynamic_index_in_dim(pieces, mine ^ h, 0, True) for h in range(group)]
        )
    )

    out = None
    for v in range(group):
        out = output_part(block_id(v), arrived[v], o_weight, width, out)
    out = out.astype(BF)
    rb = span // len(order)
    place = {o: i for i, o in enumerate(order)}
    blocks = out.reshape(len(order), rb, out.shape[1])
    where = jnp.asarray([place[o] for o in range(len(order))], jnp.int32)
    out = jnp.concatenate(
        [
            lax.dynamic_index_in_dim(blocks, where[outer ^ b], 0, False)
            for b in range(len(order))
        ]
    )
    halves = out.reshape(nh, span // nh, out.shape[1])
    me = lax.axis_index("head")
    total = lax.dynamic_index_in_dim(halves, me, 0, False).astype(F32)
    for v in range(1, nh):
        total = total + swap(
            lax.dynamic_index_in_dim(halves, me ^ v, 0, False), "head", v
        ).astype(F32)
    return (importance, total.astype(BF))


def solution(mesh):
    return jax.shard_map(
        on_device,
        mesh=mesh,
        in_specs=(
            P(None, "ctx"),
            P("ctx", "head"),
            P("head", "ctx", None),
            P("head", "ctx", None),
            P("head", "ctx"),
            P(),
        ),
        out_specs=(P("head", "ctx"), P("head", "ctx")),
        check_vma=False,
    )
```

```python
import functools
import math

import jax
import jax.numpy as jnp
from jax import lax
from jax.experimental import pallas as pl
from jax.experimental.pallas import tpu as pltpu
from jax.sharding import PartitionSpec as P


NEG = -1e30
BF = jnp.bfloat16
F32 = jnp.float32
LANES = 128


def digits_of(n):
    out, shift = [], 0
    while n > 1:
        r = 4 if n % 4 == 0 else 2
        out.append((r, shift))
        n //= r
        shift += r.bit_length() - 1
    return out


def swap(x, axis, v):
    n = lax.axis_size(axis)
    return lax.ppermute(x, axis, [(i, i ^ v) for i in range(n)])


def block_order(digits):
    order = [0]
    for r, shift in reversed(digits):
        order = [(v << shift) | o for v in range(r) for o in order]
    return order


def gather_rows(x, axis, digits, base):
    for r, shift in reversed(digits):
        x = jnp.concatenate([x] + [swap(x, axis, v << (shift + base)) for v in range(1, r)])
    return x


def permuted_rows(x, index, order):
    blocks = x.reshape(len(order), x.shape[0] // len(order), x.shape[1])
    return jnp.concatenate(
        [lax.dynamic_index_in_dim(blocks, index ^ o, 0, False) for o in order]
    )


def cdot(a, b, ca, cb):
    return lax.dot_general(a, b, (((ca,), (cb,)), ((), ())), preferred_element_type=F32)


def project_kernel(order, s_ref, h_ref, w_ref, *o_refs):
    step = pl.program_id(0)
    rb = h_ref.shape[0] // len(order)
    rows = h_ref[...]
    if len(order) > 1 and rb % 16 == 0:
        outer = s_ref[len(o_refs)]
        rows = jnp.concatenate(
            [h_ref[pl.ds(pl.multiple_of((outer ^ o) * rb, rb), rb), :] for o in order]
        )
    out = jnp.dot(rows, w_ref[...], preferred_element_type=F32)
    for i, o_ref in enumerate(o_refs):

        @pl.when(step == i)
        def _():
            o_ref[...] = out.astype(o_ref.dtype)


def project(scal, hidden, weight, width, order, dtypes):
    rows, k = hidden.shape
    return pl.pallas_call(
        functools.partial(project_kernel, order),
        out_shape=[jax.ShapeDtypeStruct((rows, width), t) for t in dtypes],
        grid_spec=pltpu.PrefetchScalarGridSpec(
            num_scalar_prefetch=1,
            grid=(len(dtypes),),
            in_specs=[
                pl.BlockSpec((rows, k), lambda i, s: (0, 0)),
                pl.BlockSpec((k, width), lambda i, s: (0, s[i])),
            ],
            out_specs=[pl.BlockSpec((rows, width), lambda i, s: (0, 0)) for _ in dtypes],
        ),
        name="query_projection",
    )(scal, hidden, weight)


def visible(s, base, limit_ref):
    pos = lax.broadcasted_iota(jnp.int32, s.shape, 0) + base
    return jnp.where(pos <= limit_ref[0:1, :], s, NEG)


def attend_kernel(n_src, bk, mb, c, s_ref, q_ref, lim_ref, *refs):
    ks, vs = refs[:n_src], refs[n_src : 2 * n_src]
    outs, (acc, peak, stat) = refs[2 * n_src : -3], refs[-3:]
    d = LANES
    heads, span = q_ref.shape[1] // d, q_ref.shape[0]

    for g in range(heads):
        acc[g] = jnp.zeros(acc.shape[1:], F32)
        peak[g] = jnp.full(peak.shape[1:], NEG, F32)

    def block(src, kb, size, masked):
        k = ks[src][pl.ds(pl.multiple_of(kb * size, size), size), :]
        each = size // mb
        vt = jnp.concatenate([vs[src][kb * each + i] for i in range(each)], axis=1)
        vt = jnp.concatenate([vt, jnp.ones((16, size), BF)])

        def scores(g):
            s = cdot(k, q_ref[:, g * d : (g + 1) * d], 1, 1)
            return visible(s, s_ref[2 * n_src + src] + kb * size, lim_ref) if masked else s

        def weigh(g, s):
            old = peak[g, 0:1, :]
            new = jnp.maximum(old, jnp.max(s, axis=0, keepdims=True))
            peak[g, 0:1, :] = new
            return jnp.exp2((s - new) * c).astype(BF), jnp.exp2((old - new) * c)

        def add(g, p, shrink):
            acc[g] = acc[g] * shrink + cdot(vt, p, 1, 0)

        s, last = scores(0), None
        for g in range(heads):
            ahead = scores(g + 1) if g + 1 < heads else None
            now = weigh(g, s)
            if last is not None:
                add(g - 1, *last)
            s, last = ahead, now
        add(heads - 1, *last)

    for src in range(n_src):
        full, some = s_ref[src], s_ref[n_src + src]
        start = full * (bk // mb)
        lax.fori_loop(0, full, lambda kb, x: (block(src, kb, bk, False), x)[1], 0)
        lax.fori_loop(start, some, lambda kb, x: (block(src, kb, mb, True), x)[1], 0)

    rb = span // len(outs)
    for g in range(heads):
        total = jnp.maximum(acc[g, d : d + 1, :], 1e-30)
        out = (acc[g, 0:d, :] / total).T.astype(BF)
        for i, o_ref in enumerate(outs):
            o_ref[:, g * d : (g + 1) * d] = out[i * rb : (i + 1) * rb]
        stat[g : g + 1, :] = peak[g, 0:1, :] * c + jnp.log2(total)

    level = stat[...]
    hi = level.astype(BF).astype(F32)
    mid = (level - hi).astype(BF).astype(F32)
    low = level - hi - mid
    pad = jnp.zeros((d - 3 * heads, span), F32)
    out = jnp.concatenate([hi, mid, low, pad]).T.astype(BF)
    for i, o_ref in enumerate(outs):
        o_ref[:, heads * d : (heads + 1) * d] = out[i * rb : (i + 1) * rb]


def attend(scal, q, limit, ks, vs, bk, mb, c, pieces):
    span, width = q.shape
    heads, n_src = width // LANES, len(ks)
    keys = ks[0].shape[0] * n_src
    vm = pl.BlockSpec(memory_space=pltpu.VMEM)
    piece = jax.ShapeDtypeStruct((span // pieces, width + LANES), BF)
    return pl.pallas_call(
        functools.partial(attend_kernel, n_src, bk, mb, c),
        out_shape=[piece] * pieces,
        in_specs=[pl.BlockSpec(memory_space=pltpu.SMEM)] + [vm] * (2 + 2 * n_src),
        out_specs=[vm] * pieces,
        scratch_shapes=[
            pltpu.VMEM((heads, LANES + 16, span), F32),
            pltpu.VMEM((heads, 8, span), F32),
            pltpu.VMEM((heads, span), F32),
        ],
        cost_estimate=pl.CostEstimate(
            flops=4 * span * heads * LANES * keys,
            transcendentals=span * heads * keys,
            bytes_accessed=2 * span * width * 2 + 4 * keys * LANES,
        ),
        name="attend",
    )(scal, q, limit, *ks, *vs)


def merge_kernel(heads, *refs):
    srcs, o_ref = refs[:-1], refs[-1]
    d = LANES

    def level_of(r):
        parts = r[:, heads * d : (heads + 1) * d].astype(F32)
        return parts + pltpu.roll(parts, d - heads, 1) + pltpu.roll(parts, d - 2 * heads, 1)

    levels = [level_of(r) for r in srcs]
    top = functools.reduce(jnp.maximum, levels)
    weights = [jnp.exp2(x - top) for x in levels]
    total = functools.reduce(jnp.add, weights)
    weights = [w / total for w in weights]
    for g in range(heads):
        o_ref[:, g * d : (g + 1) * d] = functools.reduce(
            jnp.add,
            [w[:, g : g + 1] * r[:, g * d : (g + 1) * d].astype(F32) for w, r in zip(weights, srcs)],
        ).astype(BF)
    level = top + jnp.log2(total)
    lane = lax.broadcasted_iota(jnp.int32, level.shape, 1)
    level = jnp.where(lane < heads, level, 0.0)
    hi = level.astype(BF).astype(F32)
    mid = (level - hi).astype(BF).astype(F32)
    low = level - hi - mid
    o_ref[:, heads * d : (heads + 1) * d] = (
        hi + pltpu.roll(mid, heads, 1) + pltpu.roll(low, 2 * heads, 1)
    ).astype(BF)


def merge(parts):
    shape = parts[0].shape
    return pl.pallas_call(
        functools.partial(merge_kernel, shape[1] // LANES - 1),
        out_shape=jax.ShapeDtypeStruct(shape, BF),
        name="merge",
    )(*parts)


def importance_kernel(n_src, bk, c, s_ref, q_ref, a_ref, lim_ref, *refs):
    ks, o_ref, lev = refs[:n_src], refs[n_src], refs[n_src + 1]
    d = LANES
    heads = q_ref.shape[1] // d
    parts = a_ref[:, heads * d : (heads + 1) * d].astype(F32).T
    level = parts[0:heads] + parts[heads : 2 * heads] + parts[2 * heads : 3 * heads]
    lev[...] = level * (1.0 / c)
    factor = s_ref[3 * n_src].astype(F32)
    o_ref[...] = jnp.zeros(o_ref.shape, F32)

    def block(src, kb, masked):
        k = ks[src][pl.ds(pl.multiple_of(kb * bk, bk), bk), :]
        best = None
        for g in range(heads):
            s = cdot(k, q_ref[:, g * d : (g + 1) * d], 1, 1) - lev[g : g + 1, :]
            best = s if best is None else jnp.maximum(best, s)
        if masked:
            best = visible(best, s_ref[2 * n_src + src] + kb * bk, lim_ref)
        best = functools.reduce(
            jnp.maximum, [best[:, x : x + d] for x in range(0, best.shape[1], d)]
        )
        best = jnp.max(best.T, axis=0, keepdims=True)
        o_ref[src, pl.ds(kb, 1), :] = factor * jnp.exp2(best * c)

    for src in range(n_src):
        full, some = s_ref[3 * n_src + 1 + src], s_ref[n_src + src]
        lax.fori_loop(0, full, lambda kb, x: (block(src, kb, False), x)[1], 0)
        lax.fori_loop(full, some, lambda kb, x: (block(src, kb, True), x)[1], 0)


def importance_of(scal, q, attended, limit, ks, bk, c):
    span, width = q.shape
    heads, n_src = width // LANES, len(ks)
    per_src = ks[0].shape[0]
    vm = pl.BlockSpec(memory_space=pltpu.VMEM)
    return pl.pallas_call(
        functools.partial(importance_kernel, n_src, bk, c),
        out_shape=jax.ShapeDtypeStruct((n_src, per_src // bk, bk), F32),
        in_specs=[pl.BlockSpec(memory_space=pltpu.SMEM)] + [vm] * (3 + n_src),
        out_specs=vm,
        scratch_shapes=[pltpu.VMEM((heads, span), F32)],
        cost_estimate=pl.CostEstimate(
            flops=2 * span * heads * LANES * per_src * n_src,
            transcendentals=per_src * n_src,
            bytes_accessed=2 * span * width * 2 + 2 * per_src * n_src * LANES,
        ),
        name="importance",
    )(scal, q, attended, limit, *ks)


def output_kernel(order, n_src, s_ref, *refs):
    parts, w_ref, outs = refs[:n_src], refs[n_src], refs[n_src + 1 :]
    width = parts[0].shape[1]
    out = None
    for i, a_ref in enumerate(parts):
        w = w_ref[pl.ds(pl.multiple_of(s_ref[i] * width, width), width), :]
        piece = jnp.dot(a_ref[...], w, preferred_element_type=F32)
        out = piece if out is None else out + piece
    if len(outs) == 1:
        outs[0][...] = out.astype(BF)
        return
    keep, give = outs
    rb = out.shape[0] // len(order)
    each = keep.shape[0] // rb
    outer, me = s_ref[n_src], s_ref[n_src + 1]
    for i, o in enumerate(order):
        block = outer ^ o
        half = block // each
        at = pl.ds(pl.multiple_of((block - half * each) * rb, rb), rb)

        @pl.when(half == me)
        def _():
            keep[at, :] = out[i * rb : (i + 1) * rb]

        @pl.when(half != me)
        def _():
            give[at, :] = out[i * rb : (i + 1) * rb].astype(BF)


def output(scal, parts, weight, order, halves):
    rows, cols = parts[0].shape[0], weight.shape[1]
    vm = pl.BlockSpec(memory_space=pltpu.VMEM)
    shapes = [jax.ShapeDtypeStruct((rows, cols), BF)]
    if halves:
        shapes = [jax.ShapeDtypeStruct((rows // 2, cols), t) for t in (F32, BF)]
    return pl.pallas_call(
        functools.partial(output_kernel, order, len(parts)),
        out_shape=shapes,
        in_specs=[pl.BlockSpec(memory_space=pltpu.SMEM)] + [vm] * (len(parts) + 1),
        out_specs=[vm] * len(shapes),
        name="output_projection",
    )(scal, *parts, weight)


def on_device(hidden, q_weight, keys, values, o_weight, start):
    span = hidden.shape[0]
    group, s_dev, head_size = keys.shape
    nh = lax.axis_size("head")
    n = lax.axis_size("ctx")
    width = q_weight.shape[1] // group
    c = head_size**-0.5 * math.log2(math.e)
    base = group.bit_length() - 1
    here, me = lax.axis_index("ctx"), lax.axis_index("head")
    mine, outer = here % group, here // group
    digits = digits_of(n // group)
    order = block_order(digits)
    rb = span // len(order)
    bk, mb = min(1024, s_dev), min(512, s_dev)
    count = s_dev // mb

    row_index = permuted_rows(jnp.arange(span, dtype=jnp.int32)[:, None], outer, order)
    limit = jnp.broadcast_to(start[0] + row_index.reshape(1, span), (8, span))
    offsets = jnp.stack([(here ^ v) * s_dev for v in range(group)]).astype(jnp.int32)
    reach = start[0] - offsets
    full = jnp.clip((reach + 1) // bk, 0, s_dev // bk)
    full_m = jnp.clip((reach + 1) // mb, 0, count)
    some = jnp.clip((reach + span - 1) // mb + 1, 0, count)
    scal = jnp.concatenate([full, some, offsets, start + span, full_m]).astype(jnp.int32)
    turn = list(range(1, group)) + [0]
    heads_p = jnp.stack([mine ^ v for v in turn] + [outer]).astype(jnp.int32)
    heads_o = jnp.stack([mine ^ v for v in range(group)] + [outer, me]).astype(jnp.int32)
    rows_here = hidden if rb % 16 == 0 else permuted_rows(hidden, outer, order)
    rows_here, limit, scal, heads_p, heads_o = lax.optimization_barrier(
        (rows_here, limit, scal, heads_p, heads_o)
    )

    parts = project(
        heads_p, rows_here, q_weight, width, order, [BF if v else F32 for v in turn]
    )
    value_t = values.reshape(group, count, mb, head_size).transpose(0, 1, 3, 2)
    k_own = lax.dynamic_index_in_dim(keys, mine, 0, False)
    v_own = lax.dynamic_index_in_dim(value_t, mine, 0, False)
    sends = [lax.dynamic_index_in_dim(keys, mine ^ v, 0, False) for v in range(1, group)]
    vsends = [lax.dynamic_index_in_dim(value_t, mine ^ v, 0, False) for v in range(1, group)]
    got = [swap(parts[v - 1], "ctx", v) for v in range(1, group)]
    ks = [k_own] + [swap(x, "ctx", v + 1) for v, x in enumerate(sends)]
    vs = [v_own] + [swap(x, "ctx", v + 1) for v, x in enumerate(vsends)]
    query = functools.reduce(jnp.add, [g.astype(F32) for g in got], parts[-1])

    for r, shift in digits:
        pieces = jnp.split(query, r)
        got = [swap(pieces[v].astype(BF), "ctx", v << (shift + base)) for v in range(1, r)]
        query = functools.reduce(jnp.add, [g.astype(F32) for g in got], pieces[0])
    query = gather_rows(query.astype(BF), "ctx", digits, base)

    pieces = attend(scal, query, limit, ks, vs, bk, mb, c, digits[0][0] if digits else 1)
    part = pieces[0]
    for i, (r, shift) in enumerate(digits):
        if i:
            pieces = jnp.split(part, r)
        got = [swap(pieces[v], "ctx", v << (shift + base)) for v in range(1, r)]
        part = merge([pieces[0]] + got)
    attended = gather_rows(part, "ctx", digits, base)

    own = attended[:, :width]
    arrived = [own] + [swap(own, "ctx", v) for v in range(1, group)]
    scores = importance_of(scal, query, attended, limit, ks, mb, c)
    pieces = [scores[v].reshape(1, s_dev) for v in range(group)]
    pieces = jnp.concatenate([pieces[0]] + [swap(pieces[v], "ctx", v) for v in range(1, group)])
    importance = jnp.concatenate(
        [lax.dynamic_index_in_dim(pieces, mine ^ h, 0, True) for h in range(group)]
    )

    halves = nh == 2 and rb % 16 == 0 and (span // nh) % rb == 0
    out = output(heads_o, arrived, o_weight, order, halves)
    if halves:
        total = out[0] + swap(out[1], "head", 1).astype(F32)
        return (importance, total.astype(BF))
    place = {o: i for i, o in enumerate(order)}
    where = jnp.asarray([place[o] for o in range(len(order))], jnp.int32)
    blocks = out[0].reshape(len(order), rb, -1)
    out = jnp.concatenate(
        [lax.dynamic_index_in_dim(blocks, where[outer ^ b], 0, False) for b in range(len(order))]
    )
    shares = out.reshape(nh, span // nh, -1)
    total = lax.dynamic_index_in_dim(shares, me, 0, False).astype(F32)
    for v in range(1, nh):
        share = lax.dynamic_index_in_dim(shares, me ^ v, 0, False)
        total = total + swap(share, "head", v).astype(F32)
    return (importance, total.astype(BF))


def solution(mesh):
    return jax.shard_map(
        on_device,
        mesh=mesh,
        in_specs=(
            P(None, "ctx"),
            P("ctx", "head"),
            P("head", "ctx", None),
            P("head", "ctx", None),
            P("head", "ctx"),
            P(),
        ),
        out_specs=(P("head", "ctx"), P("head", "ctx")),
        check_vma=False,
    )
```
